32 devices in a mesh: grp: 2 (over y), tok: 4 (over z), feat: 4 (over x, core).
Axes of the slice: x: 2, y: 2, z: 4, core: 2. Of those that a mesh axis runs over, the one named last changes fastest.
Arguments:
- acts: bfloat16 [6144, 28672], P(('grp', 'tok'), 'feat'), parts along dimension 0, may hold values from -6 to 6
- grads: bfloat16 [6144, 8192], P(('grp', 'tok'), 'feat'), parts along dimension 0, may hold values from -6 to 6
- proj_in: bfloat16 [28672, 512], P('feat'), may hold values from -0.03125 to 0.03125
- proj_out: bfloat16 [8192, 512], P('feat'), may hold values from -0.0625 to 0.0625
- doc_lengths: int32 [8], P('grp'), parts along dimension 0, may hold values from 1 to 1536, 3072 in all
- doc_owner: int32 [8], P('grp'), parts along dimension 0, may hold values from 0 to 3, as said below
Outputs:
- doc_grads: float32 [8, 512, 512], P(('grp', 'tok'), 'feat'), parts along dimension 0
The draws below stay inside these ranges and needn't reach their ends.
There are 2 independent parts, one for each index of `grp`. The reference program is written for one: setup_inputs(seed, part) draws one part's arguments, and reference() takes and returns one part's arrays. A program takes and returns all parts, laid end to end along the dimension named above; an argument that names none is the same for every part. Nothing has to cross between parts.
Inputs may be any that keep to these rules, and one draw needn't show every extreme that they name: `doc_lengths`: the lengths sum to 3072; the largest is exactly 1536. `doc_owner`: every index along tok owns exactly 1 documents.
All inputs are finite; a program needn't handle non-finite values.
Results may differ from the reference program's by a relative error of at most 0.0043.
Values may be sent and summed in bfloat16 or wider, within the bound.
No kernel may reach another device: no remote copies, remote signals or barrier semaphores. Data moves between devices by JAX's collectives and lax.ppermute only.
A program may use at most 64 MiB of HBM per device.

```python
import math
import jax
import jax.numpy as jnp
import numpy as np
from jax import lax

DIN = 28672
DOUT = 8192
RANK = 512
DOC_SLOTS = 1
TOKENS = 3072
DOCS = 4
LEN_MOST = 1536


def draw_doc_owner(key, part):
    shuffled = jax.random.permutation(jax.random.fold_in(key, 11), DOCS)
    return (shuffled // DOC_SLOTS).astype(jnp.int32)


def shard_levels(rng, extent, shards, low, high):
    def one(dim, shards_of):
        heights = jax.random.uniform(jax.random.fold_in(jax.random.fold_in(rng, 6), dim), (shards_of,), jnp.float32, low / len(shards), high / len(shards))
        return jnp.repeat(jnp.exp(heights), extent[dim] // shards_of).reshape((-1,) + (1,) * (len(extent) - dim - 1))

    level = one(*shards[0])
    for cut in shards[1:]:
        level = level * one(*cut)
    return level


def split_up(amount, total, reach, lean):
    weights = [(1 << 20) // math.isqrt(rank ** lean) + 1 for rank in range(2, amount + 1)]
    spare, holding = total - reach - (amount - 1), [1] * (amount - 1)
    while spare > 0:
        movable = [i for i in range(amount - 1) if holding[i] < reach]
        whole, remaining = sum([weights[i] for i in movable]), spare
        for i in movable:
            addition = min(reach - holding[i], max(1, remaining * weights[i] // whole), spare)
            holding[i] = holding[i] + addition
            spare = spare - addition
    return np.array([reach] + holding)


def ragged_sizes(own_key, number_of, total, reach, lean):
    if number_of == 2:
        one = jax.random.randint(own_key, (), max(1, total - reach), min(reach, total - 1) + 1)
        return jnp.stack([one, total - one])
    lengths = jnp.asarray(split_up(number_of, total, reach, lean), jnp.int32)
    couples = (number_of - 1) // 2
    giver, taker = lengths[1:1 + 2 * couples:2], lengths[2:2 + 2 * couples:2]
    slack = jnp.minimum(giver - 1, reach - taker)
    shifted = jax.random.randint(jax.random.fold_in(own_key, 1), (couples,), 0, 1 << 20) % (slack + 1)
    lengths = lengths.at[1:1 + 2 * couples:2].set(giver - shifted).at[2:2 + 2 * couples:2].set(taker + shifted)
    return lengths[jax.random.permutation(jax.random.fold_in(own_key, 2), number_of)]


def centred(own_key, dims, width, reach, split=(), held_as=jnp.bfloat16):
    entries = jax.random.normal(own_key, dims, jnp.float32) * width
    if len(split) > 0:
        entries = shard_levels(own_key, dims, split, -0.22, 0.18) * entries
    return jnp.clip(entries, min=-reach, max=reach).astype(held_as)


def setup_inputs(seed: int = 0, part: int = 0) -> dict:
    key_of = jax.random.split(jax.random.key(seed), 7)
    own_keys = jax.random.split(jax.random.fold_in(key_of[6], part), 7)
    return {
        "acts": centred(own_keys[0], (TOKENS, DIN), 1.0, 6.0, ((0, 4), (1, 4))),
        "grads": centred(own_keys[1], (TOKENS, DOUT), 1.0, 6.0, ((0, 4), (1, 4))),
        "proj_in": centred(key_of[2], (DIN, RANK), DIN ** -0.5, 0.03125, ((0, 4),)),
        "proj_out": centred(key_of[3], (DOUT, RANK), DOUT ** -0.5, 0.0625, ((0, 4),)),
        "doc_lengths": ragged_sizes(own_keys[4], DOCS, TOKENS, LEN_MOST, 2).astype(jnp.int32),
        "doc_owner": draw_doc_owner(jax.random.fold_in(jax.random.fold_in(key_of[6], part), 71), part),
    }


def reference(acts, grads, proj_in, proj_out, doc_lengths, doc_owner):
    inputs_low = jnp.dot(acts, proj_in, preferred_element_type=jnp.float32).astype(jnp.bfloat16)
    grads_low = jnp.dot(grads, proj_out, preferred_element_type=jnp.float32).astype(jnp.bfloat16)
    doc_ends = jnp.cumsum(doc_lengths).astype(jnp.int32)
    doc_starts = (doc_ends - doc_lengths).astype(jnp.int32)
    position = jnp.arange(acts.shape[0], dtype=jnp.int32)

    def one_doc(bounds):
        start_at, end_at = bounds
        member = ((position >= start_at) & (position < end_at)).astype(grads_low.dtype)
        weighted = grads_low * member[:, None]
        return jnp.dot(weighted.T, inputs_low, preferred_element_type=jnp.float32)
    gradients = lax.map(one_doc, (doc_starts, doc_ends))
    gradients = gradients * lax.rsqrt(doc_lengths.astype(jnp.float32))[:, None, None]
    doc_index = jnp.arange(doc_owner.shape[0], dtype=jnp.int32)
    same_owner = doc_owner[:, None] == doc_owner[None, :]
    earlier = doc_index[:, None] < doc_index[None, :]
    slot_rank = lax.optimization_barrier(jnp.sum((same_owner & earlier).astype(jnp.int32), axis=0)).astype(jnp.int32)
    target = (doc_owner * DOC_SLOTS + slot_rank).astype(jnp.int32)
    return jnp.zeros_like(gradients).at[target].set(gradients)
```

```python
import functools

import jax
import jax.numpy as jnp
from jax import lax
from jax.experimental import pallas as pl
from jax.experimental.pallas import tpu as pltpu
from jax.sharding import PartitionSpec as P


CHUNKS = 2
FIRST = 2
MIB = 1 << 20


def partner_pairs(size):
    return [(i, i ^ 1) for i in range(size)]


def chip_shift(size, step):
    chips = size // 2
    return [(i, ((i // 2 + step) % chips) * 2 + i % 2) for i in range(size)]


def exchange(size, step):
    if size & (size - 1) == 0:
        return [(i, i ^ step) for i in range(size)]
    return [(i, (i + step) % size) for i in range(size)]


def receiver(size, me, step):
    return me ^ step if size & (size - 1) == 0 else (me + step) % size


def depth_tile(depth, most):
    tile = most // 128 * 128
    while depth % tile:
        tile -= 128
    return tile


def split_by_core(core, product, share, groups, mine_ref, theirs_ref):
    for which in range(2):

        @pl.when(core == which)
        def _():
            for group in range(groups):
                place = pl.ds(group * share, share)
                mine_ref[:, place] = product[:, pl.ds((2 * group + which) * share, share)]
                theirs_ref[:, place] = product[:, pl.ds((2 * group + 1 - which) * share, share)]


def grads_kernel(chips, core_ref, a_hbm, w_hbm, mine_ref, theirs_ref, a_ref, w_ref, total, sems):
    depth, rank = w_ref.shape
    tile = depth_tile(depth, 512)
    copies = []
    for t in range(depth // tile):
        lines = pl.ds(t * tile, tile)
        group = (
            pltpu.make_async_copy(a_hbm.at[:, lines], a_ref.at[:, lines], sems.at[0, t]),
            pltpu.make_async_copy(w_hbm.at[lines, :], w_ref.at[lines, :], sems.at[1, t]),
        )
        for copy in group:
            copy.start()
        copies.append(group)
    for t in range(depth // tile):
        lines = pl.ds(t * tile, tile)
        for copy in copies[t]:
            copy.wait()
        product = jnp.dot(a_ref[:, lines], w_ref[lines, :], preferred_element_type=jnp.float32)
        if t == 0:
            total[...] = product
        else:
            total[...] += product
    split_by_core(core_ref[0], total, rank // (2 * chips), chips, mine_ref, theirs_ref)


def project_grads(grads, proj_out, core, chips):
    rows, depth = grads.shape
    rank = proj_out.shape[1]
    count = depth // depth_tile(depth, 512)
    half = pltpu.VMEM((rows, rank // 2), jnp.float32)
    return pl.pallas_call(
        functools.partial(grads_kernel, chips),
        in_specs=[pl.BlockSpec(memory_space=pltpu.SMEM)]
        + [pl.BlockSpec(memory_space=pltpu.HBM)] * 2,
        out_specs=[pl.BlockSpec(memory_space=pltpu.VMEM)] * 2,
        out_shape=[half, half],
        scratch_shapes=[
            pltpu.VMEM((rows, depth), grads.dtype),
            pltpu.VMEM((depth, rank), proj_out.dtype),
            pltpu.VMEM((rows, rank), jnp.float32),
            pltpu.SemaphoreType.DMA((2, count)),
        ],
        compiler_params=pltpu.CompilerParams(vmem_limit_bytes=12 * MIB),
        cost_estimate=pl.CostEstimate(
            flops=2 * rows * depth * rank,
            bytes_accessed=2 * (rows * depth + depth * rank),
            transcendentals=0,
        ),
        name="project_grads",
    )(core, grads, proj_out)


def acts_kernel(first, last, begin, core_ref, a_hbm, w_hbm, *refs):
    refs = list(refs)
    refs.pop(0)
    start_ref = None if first else refs.pop(0)
    a_ref, w_ref, total, sems = refs[-4:]
    out_refs = refs[:-4]
    span = w_ref.shape[0]
    tile = depth_tile(span, 1024)
    copies = []
    for t in range(span // tile):
        lines = pl.ds(t * tile, tile)
        far_lines = pl.ds(begin + t * tile, tile)
        group = (
            pltpu.make_async_copy(a_hbm.at[:, far_lines], a_ref.at[:, lines], sems.at[0, t]),
            pltpu.make_async_copy(w_hbm.at[far_lines, :], w_ref.at[lines, :], sems.at[1, t]),
        )
        for copy in group:
            copy.start()
        copies.append(group)
    into = total if last else out_refs[0]
    for t in range(span // tile):
        lines = pl.ds(t * tile, tile)
        for copy in copies[t]:
            copy.wait()
        product = jnp.dot(a_ref[:, lines], w_ref[lines, :], preferred_element_type=jnp.float32)
        if t > 0:
            into[...] += product
        elif first:
            into[...] = product
        else:
            into[...] = start_ref[...] + product
    if last:
        chunks = len(out_refs) // 2
        half, width = out_refs[0].shape
        for chunk in range(chunks):
            columns = pl.ds(chunk * width, width)
            own = pl.ds(pl.multiple_of(core_ref[0] * half, half), half)
            other = pl.ds(pl.multiple_of((1 - core_ref[0]) * half, half), half)
            out_refs[2 * chunk][...] = total[own, columns]
            out_refs[2 * chunk + 1][...] = total[other, columns]


def project_acts(acts, proj_in, core, begin, span, after, start, chunks):
    rows, rank = acts.shape[0], proj_in.shape[1]
    first, last = start is None, begin + span == proj_in.shape[0]
    if last:
        out = [pltpu.VMEM((rows // 2, rank // chunks), jnp.float32)] * (2 * chunks)
    else:
        out = [pltpu.VMEM((rows, rank), jnp.float32)]
    starts = [] if first else [start]
    return pl.pallas_call(
        functools.partial(acts_kernel, first, last, begin),
        in_specs=[pl.BlockSpec(memory_space=pltpu.SMEM)]
        + [pl.BlockSpec(memory_space=pltpu.HBM)] * 2
        + [pl.BlockSpec(memory_space=pl.ANY)]
        + [pl.BlockSpec(memory_space=pltpu.VMEM)] * len(starts),
        out_specs=[pl.BlockSpec(memory_space=pltpu.VMEM)] * len(out),
        out_shape=out,
        scratch_shapes=[
            pltpu.VMEM((rows, span), acts.dtype),
            pltpu.VMEM((span, rank), proj_in.dtype),
            pltpu.VMEM((rows, rank), jnp.float32),
            pltpu.SemaphoreType.DMA((2, span // depth_tile(span, 1024))),
        ],
        compiler_params=pltpu.CompilerParams(vmem_limit_bytes=24 * MIB),
        cost_estimate=pl.CostEstimate(
            flops=2 * rows * span * rank,
            bytes_accessed=2 * span * (rank + rows),
            transcendentals=0,
        ),
        name="project_acts",
    )(core, acts, proj_in, after, *starts)


def spread_kernel(tok_count, core_ref, tok_ref, lengths_ref, owner_ref, low_ref, out_ref):
    rows, share = low_ref.shape
    docs = lengths_ref.shape[0]
    slots = docs // tok_count
    half = rows // 2
    tok, core = tok_ref[0], core_ref[0]
    starts, ends, targets = [], [], []
    seen = jnp.int32(0)
    for d in range(docs):
        starts.append(seen)
        seen = seen + lengths_ref[d]
        ends.append(seen)
        rank = jnp.int32(0)
        for e in range(d):
            rank = rank + (owner_ref[e] == owner_ref[d]).astype(jnp.int32)
        targets.append(owner_ref[d] * slots + rank)
    turned = low_ref[...].astype(jnp.float32).T
    for part in range(2):
        first = (core if part == 0 else 1 - core) * half
        position = tok * rows + first + lax.broadcasted_iota(jnp.int32, (share, half), 1)
        piece = jnp.where(
            core == part, turned[:, :half], turned[:, half:]
        )
        for step in range(tok_count):
            for slot in range(slots):
                want = receiver(tok_count, tok, step) * slots + slot
                begin = end = jnp.int32(0)
                for d in range(docs):
                    hit = targets[d] == want
                    begin = jnp.where(hit, starts[d], begin)
                    end = jnp.where(hit, ends[d], end)
                member = (position >= begin) & (position < end)
                out_ref[pl.ds((step * slots + slot) * share, share), pl.ds(part * half, half)] = (
                    jnp.where(member, piece, 0.0).astype(out_ref.dtype)
                )


def spread(low, core, tok, doc_lengths, doc_owner, tok_count):
    rows, share = low.shape
    docs = doc_lengths.shape[0]
    return pl.pallas_call(
        functools.partial(spread_kernel, tok_count),
        in_specs=[pl.BlockSpec(memory_space=pltpu.SMEM)] * 4
        + [pl.BlockSpec(memory_space=pltpu.VMEM)],
        out_specs=pl.BlockSpec(memory_space=pltpu.VMEM),
        out_shape=pltpu.VMEM((docs * share, rows), jnp.bfloat16),
        compiler_params=pltpu.CompilerParams(vmem_limit_bytes=6 * MIB),
        cost_estimate=pl.CostEstimate(flops=10**6, bytes_accessed=0, transcendentals=0),
        name="spread",
    )(core, tok, doc_lengths, doc_owner, low)


def product_kernel(w_ref, own_ref, other_ref, kept_ref, *sent_refs):
    half = own_ref.shape[0]
    size = kept_ref.shape[0]
    product = jnp.dot(w_ref[:, :half], own_ref[...], preferred_element_type=jnp.float32)
    product += jnp.dot(w_ref[:, half:], other_ref[...], preferred_element_type=jnp.float32)
    kept_ref[...] = product[:size]
    for i, ref in enumerate(sent_refs):
        ref[...] = product[(i + 1) * size : (i + 2) * size].astype(ref.dtype)


def outer_products(spread_low, own, other, tok_count):
    size = spread_low.shape[0] // tok_count
    width = own.shape[1]
    return pl.pallas_call(
        product_kernel,
        in_specs=[pl.BlockSpec(memory_space=pltpu.VMEM)] * 3,
        out_specs=[pl.BlockSpec(memory_space=pltpu.VMEM)] * tok_count,
        out_shape=[pltpu.VMEM((size, width), jnp.float32)]
        + [pltpu.VMEM((size, width), jnp.bfloat16)] * (tok_count - 1),
        compiler_params=pltpu.CompilerParams(vmem_limit_bytes=6 * MIB),
        cost_estimate=pl.CostEstimate(
            flops=2 * spread_low.shape[0] * spread_low.shape[1] * width,
            bytes_accessed=0,
            transcendentals=0,
        ),
        name="outer_products",
    )(spread_low, own, other)


def finish_kernel(tok_count, tok_ref, lengths_ref, owner_ref, *refs):
    total_refs, out_ref = refs[:-1], refs[-1]
    docs = lengths_ref.shape[0]
    slots = docs // tok_count
    share = out_ref.shape[1]
    tok = tok_ref[0]
    for slot in range(slots):
        length = jnp.int32(0)
        for d in range(docs):
            rank = jnp.int32(0)
            for e in range(d):
                rank = rank + (owner_ref[e] == owner_ref[d]).astype(jnp.int32)
            hit = (owner_ref[d] == tok) & (rank == slot)
            length = jnp.where(hit, lengths_ref[d], length)
        place = 0
        for chunk in range(CHUNKS):
            parts = total_refs[chunk * tok_count : (chunk + 1) * tok_count]
            width = parts[0].shape[1]
            lines = pl.ds(slot * share, share)
            total = parts[0][lines, :]
            for part in parts[1:]:
                total = total + part[lines, :].astype(jnp.float32)
            scaling = lax.rsqrt(jnp.full((share, width), length, jnp.int32).astype(jnp.float32))
            out_ref[slot, :, pl.ds(place, width)] = total * scaling
            place += width


def finish(parts, tok, doc_lengths, doc_owner, tok_count, share):
    slots = doc_lengths.shape[0] // tok_count
    rank = sum(p.shape[1] for p in parts[::tok_count])
    return pl.pallas_call(
        functools.partial(finish_kernel, tok_count),
        in_specs=[pl.BlockSpec(memory_space=pltpu.SMEM)] * 3
        + [pl.BlockSpec(memory_space=pltpu.VMEM)] * len(parts),
        out_specs=pl.BlockSpec(memory_space=pltpu.VMEM),
        out_shape=jax.ShapeDtypeStruct((slots, share, rank), jnp.float32),
        compiler_params=pltpu.CompilerParams(vmem_limit_bytes=6 * MIB),
        name="finish",
    )(tok, doc_lengths, doc_owner, *parts)


def shards(acts, grads, proj_in, proj_out, doc_lengths, doc_owner):
    depth, rank = proj_in.shape
    tok_count = lax.axis_size("tok")
    feat_count = lax.axis_size("feat")
    chips = feat_count // 2
    feat = lax.axis_index("feat")
    chip = feat // 2
    core = (feat % 2).reshape(1)
    tok = lax.axis_index("tok").reshape(1)
    share = rank // feat_count
    first = depth // 7 * FIRST
    acts, grads, proj_in, proj_out = (
        pltpu.with_memory_space_constraint(v, pltpu.HBM) for v in (acts, grads, proj_in, proj_out)
    )

    def swap(value):
        return lax.ppermute(value, "feat", partner_pairs(feat_count))

    mine, theirs = project_grads(grads, proj_out, core, chips)
    other = swap(theirs)
    pair_out = mine + other
    out_low = lax.dynamic_slice_in_dim(pair_out, chip * share, share, 1)
    sent = [
        lax.dynamic_slice_in_dim(
            pair_out, (chip + step) % chips * share, share, 1
        ).astype(jnp.bfloat16)
        for step in range(1, chips)
    ]
    next_after = sent[0]
    for step in range(1, chips):
        other = lax.ppermute(sent[step - 1], "feat", chip_shift(feat_count, step))
        out_low = out_low + other.astype(jnp.float32)
    out_low = out_low.astype(jnp.bfloat16)

    (held,) = project_acts(acts, proj_in, core, 0, first, theirs, None, CHUNKS)
    halves = project_acts(
        acts, proj_in, core, first, depth - first, next_after, held, CHUNKS
    )
    lows = []
    for chunk in range(CHUNKS):
        mine, theirs = halves[2 * chunk : 2 * chunk + 2]
        other = swap(theirs)
        pair_in = mine + other
        sent = pair_in.astype(jnp.bfloat16)
        full_in = pair_in
        for step in range(1, chips):
            other = lax.ppermute(sent, "feat", chip_shift(feat_count, step))
            full_in = full_in + other.astype(jnp.float32)
        lows.append(full_in.astype(jnp.bfloat16))

    spread_low = spread(out_low, core, tok, doc_lengths, doc_owner, tok_count)
    parts = []
    for low_in in lows:
        other = swap(low_in)
        kept, *sends = outer_products(spread_low, low_in, other, tok_count)
        parts.append(kept)
        for step in range(1, tok_count):
            parts.append(lax.ppermute(sends[step - 1], "tok", exchange(tok_count, step)))
    return finish(parts, tok, doc_lengths, doc_owner, tok_count, share)


def solution(mesh):
    in_specs = (
        P(("grp", "tok"), "feat"),
        P(("grp", "tok"), "feat"),
        P("feat", None),
        P("feat", None),
        P("grp"),
        P("grp"),
    )
    out_specs = P(("grp", "tok"), "feat", None)

    return jax.shard_map(shards, mesh=mesh, in_specs=in_specs, out_specs=out_specs, check_vma=False)
```

```python
import functools

import jax
import jax.numpy as jnp
from jax import lax
from jax.experimental import pallas as pl
from jax.experimental.pallas import tpu as pltpu
from jax.sharding import PartitionSpec as P


CHUNKS = 2
TILE = 512
AHEAD = 8
MIB = 1 << 20


def partner_pairs(size):
    return [(i, i ^ 1) for i in range(size)]


def chip_shift(size, step):
    chips = size // 2
    return [(i, ((i // 2 + step) % chips) * 2 + i % 2) for i in range(size)]


def exchange(size, step):
    if size & (size - 1) == 0:
        return [(i, i ^ step) for i in range(size)]
    return [(i, (i + step) % size) for i in range(size)]


def receiver(size, me, step):
    return me ^ step if size & (size - 1) == 0 else (me + step) % size


def depth_tile(depth, most):
    tile = most // 128 * 128
    while depth % tile:
        tile -= 128
    return tile


def stream(far, near, far_w, near_w, sems):
    depth = near_w.shape[0]
    tile = depth_tile(depth, TILE)
    count = depth // tile

    def lines(t):
        return pl.ds(t * tile, tile)

    def copies(t):
        return (
            pltpu.make_async_copy(far_w.at[lines(t), :], near_w.at[lines(t), :], sems.at[0, t]),
            pltpu.make_async_copy(far.at[:, lines(t)], near.at[:, lines(t)], sems.at[1, t]),
        )

    def start(t):
        for copy in copies(t):
            copy.start()

    for t in range(min(AHEAD, count)):
        start(t)
    for t in range(count):
        for copy in copies(t):
            copy.wait()
        if t + AHEAD < count:
            start(t + AHEAD)
        yield lines(t), t == 0, t + 1 == count


def grads_kernel(chips, chip_ref, a_hbm, w_hbm, near_ref, *refs):
    far_refs, (a_ref, w_ref, total, sems) = refs[:-4], refs[-4:]
    for lines, begins, _ in stream(a_hbm, a_ref, w_hbm, w_ref, sems):
        product = jnp.dot(a_ref[:, lines], w_ref[lines, :], preferred_element_type=jnp.float32)
        if begins:
            total[...] = product
        else:
            total[...] += product
    width = near_ref.shape[1]
    for chip in range(chips):

        @pl.when(chip_ref[0] == chip)
        def _():
            near_ref[...] = total[:, pl.ds(chip * width, width)]
            for step, ref in enumerate(far_refs):
                place = (chip + step + 1) % chips * width
                ref[...] = total[:, pl.ds(place, width)].astype(ref.dtype)


def acts_kernel(core_ref, a_hbm, w_hbm, after_ref, *refs):
    halves, (a_ref, w_ref, total, sems) = refs[:-4], refs[-4:]
    half, width = halves[0].shape
    for lines, begins, ends in stream(a_hbm, a_ref, w_hbm, w_ref, sems):
        if not ends:
            product = jnp.dot(a_ref[:, lines], w_ref[lines, :], preferred_element_type=jnp.float32)
            if begins:
                total[...] = product
            else:
                total[...] += product
            continue
        for side in range(2):
            place = core_ref[0] if side == 0 else 1 - core_ref[0]
            rows = pl.ds(pl.multiple_of(place * half, half), half)
            result = jnp.dot(a_ref[rows, lines], w_ref[lines, :], preferred_element_type=jnp.float32)
            if not begins:
                result = total[rows, :] + result
            for chunk in range(len(halves) // 2):
                halves[2 * chunk + side][...] = result[:, chunk * width : (chunk + 1) * width]


def product_call(kernel, scalar, a, w, after, out):
    rows, depth = a.shape
    rank = w.shape[1]
    return pl.pallas_call(
        kernel,
        in_specs=[pl.BlockSpec(memory_space=pltpu.SMEM)]
        + [pl.BlockSpec(memory_space=pltpu.HBM)] * 2
        + [pl.BlockSpec(memory_space=pl.ANY)] * len(after),
        out_specs=[pl.BlockSpec(memory_space=pltpu.VMEM)] * len(out),
        out_shape=out,
        scratch_shapes=[
            pltpu.VMEM((rows, depth), a.dtype),
            pltpu.VMEM((depth, rank), w.dtype),
            pltpu.VMEM((rows, rank), jnp.float32),
            pltpu.SemaphoreType.DMA((2, depth // depth_tile(depth, TILE))),
        ],
        compiler_params=pltpu.CompilerParams(
            vmem_limit_bytes=2 * depth * (rows + rank) + 4 * rows * rank + 3 * MIB
        ),
        cost_estimate=pl.CostEstimate(
            flops=2 * rows * depth * rank,
            bytes_accessed=2 * (rows + rank) * depth,
            transcendentals=0,
        ),
    )(scalar, a, w, *after)


def project_grads(grads, proj_out, chip, chips):
    rows, rank = grads.shape[0], proj_out.shape[1]
    width = rank // chips
    out = [pltpu.VMEM((rows, width), jnp.float32)]
    out += [pltpu.VMEM((rows, width), jnp.bfloat16)] * (chips - 1)
    return product_call(functools.partial(grads_kernel, chips), chip, grads, proj_out, [], out)


def project_acts(acts, proj_in, core, after):
    rows, rank = acts.shape[0], proj_in.shape[1]
    out = [pltpu.VMEM((rows // 2, rank // CHUNKS), jnp.float32)] * (2 * CHUNKS)
    return product_call(acts_kernel, core, acts, proj_in, [after], out)


def vmem_call(kernel, scalars, arrays, out, limit=6, flops=10**5):
    arrays = [pltpu.with_memory_space_constraint(v, pltpu.VMEM) for v in arrays]
    return pl.pallas_call(
        kernel,
        in_specs=[pl.BlockSpec(memory_space=pltpu.SMEM)] * len(scalars)
        + [pl.BlockSpec(memory_space=pltpu.VMEM)] * len(arrays),
        out_specs=[pl.BlockSpec(memory_space=pltpu.VMEM)] * len(out),
        out_shape=out,
        compiler_params=pltpu.CompilerParams(vmem_limit_bytes=limit * MIB),
        cost_estimate=pl.CostEstimate(flops=flops, bytes_accessed=0, transcendentals=0),
    )(*scalars, *arrays)


def chip_sum_kernel(core_ref, near_ref, *refs):
    far_refs, (mine_ref, theirs_ref) = refs[:-2], refs[-2:]
    share = mine_ref.shape[1]
    for which in range(2):

        @pl.when(core_ref[0] == which)
        def _():
            for side, out_ref in ((which, mine_ref), (1 - which, theirs_ref)):
                place = pl.ds(side * share, share)
                total = near_ref[:, place]
                for ref in far_refs:
                    total = total + ref[:, place].astype(jnp.float32)
                out_ref[...] = total


def pair_sum_kernel(mine_ref, other_ref, total_ref, sent_ref):
    total = mine_ref[...] + other_ref[...]
    total_ref[...] = total
    sent_ref[...] = total.astype(sent_ref.dtype)


def spread_kernel(
    tok_count, core_ref, tok_ref, lengths_ref, owner_ref, mine_ref, other_ref, out_ref
):
    rows, share = mine_ref.shape
    docs = lengths_ref.shape[0]
    slots = docs // tok_count
    half = rows // 2
    tok, core = tok_ref[0], core_ref[0]
    starts, ends, targets = [], [], []
    seen = jnp.int32(0)
    for d in range(docs):
        starts.append(seen)
        seen = seen + lengths_ref[d]
        ends.append(seen)
        rank = jnp.int32(0)
        for e in range(d):
            rank = rank + (owner_ref[e] == owner_ref[d]).astype(jnp.int32)
        targets.append(owner_ref[d] * slots + rank)
    low = (mine_ref[...] + other_ref[...]).astype(jnp.bfloat16)
    turned = low.astype(jnp.float32).T
    for part in range(2):
        first = (core if part == 0 else 1 - core) * half
        position = tok * rows + first + lax.broadcasted_iota(jnp.int32, (share, half), 1)
        piece = jnp.where(
            core == part, turned[:, :half], turned[:, half:]
        )
        for step in range(tok_count):
            for slot in range(slots):
                want = receiver(tok_count, tok, step) * slots + slot
                begin = end = jnp.int32(0)
                for d in range(docs):
                    hit = targets[d] == want
                    begin = jnp.where(hit, starts[d], begin)
                    end = jnp.where(hit, ends[d], end)
                member = (position >= begin) & (position < end)
                out_ref[pl.ds((step * slots + slot) * share, share), pl.ds(part * half, half)] = (
                    jnp.where(member, piece, 0.0).astype(out_ref.dtype)
                )


def spread(mine, other, core, tok, doc_lengths, doc_owner, tok_count):
    rows, share = mine.shape
    out = pltpu.VMEM((doc_lengths.shape[0] * share, rows), jnp.bfloat16)
    (result,) = vmem_call(
        functools.partial(spread_kernel, tok_count),
        (core, tok, doc_lengths, doc_owner),
        (mine, other),
        [out],
        limit=8,
    )
    return result


def product_kernel(w_ref, own_ref, other_ref, kept_ref, *sent_refs):
    half = own_ref.shape[0]
    size = kept_ref.shape[0]
    product = jnp.dot(w_ref[:, :half], own_ref[...], preferred_element_type=jnp.float32)
    product += jnp.dot(w_ref[:, half:], other_ref[...], preferred_element_type=jnp.float32)
    kept_ref[...] = product[:size]
    for i, ref in enumerate(sent_refs):
        ref[...] = product[(i + 1) * size : (i + 2) * size].astype(ref.dtype)


def outer_products(spread_low, own, other, tok_count):
    size = spread_low.shape[0] // tok_count
    width = own.shape[1]
    return pl.pallas_call(
        product_kernel,
        in_specs=[pl.BlockSpec(memory_space=pltpu.VMEM)] * 3,
        out_specs=[pl.BlockSpec(memory_space=pltpu.VMEM)] * tok_count,
        out_shape=[pltpu.VMEM((size, width), jnp.float32)]
        + [pltpu.VMEM((size, width), jnp.bfloat16)] * (tok_count - 1),
        compiler_params=pltpu.CompilerParams(vmem_limit_bytes=6 * MIB),
        cost_estimate=pl.CostEstimate(
            flops=2 * spread_low.shape[0] * spread_low.shape[1] * width,
            bytes_accessed=0,
            transcendentals=0,
        ),
        name="outer_products",
    )(spread_low, own, other)


def finish_kernel(tok_count, tok_ref, lengths_ref, owner_ref, *refs):
    total_refs, out_ref = refs[:-1], refs[-1]
    docs = lengths_ref.shape[0]
    slots = docs // tok_count
    share = out_ref.shape[1]
    tok = tok_ref[0]
    for slot in range(slots):
        length = jnp.int32(0)
        for d in range(docs):
            rank = jnp.int32(0)
            for e in range(d):
                rank = rank + (owner_ref[e] == owner_ref[d]).astype(jnp.int32)
            hit = (owner_ref[d] == tok) & (rank == slot)
            length = jnp.where(hit, lengths_ref[d], length)
        place = 0
        for chunk in range(CHUNKS):
            parts = total_refs[chunk * tok_count : (chunk + 1) * tok_count]
            width = parts[0].shape[1]
            lines = pl.ds(slot * share, share)
            total = parts[0][lines, :]
            for part in parts[1:]:
                total = total + part[lines, :].astype(jnp.float32)
            scaling = lax.rsqrt(jnp.full((share, width), length, jnp.int32).astype(jnp.float32))
            out_ref[slot, :, pl.ds(place, width)] = total * scaling
            place += width


def finish(parts, tok, doc_lengths, doc_owner, tok_count, share):
    slots = doc_lengths.shape[0] // tok_count
    rank = sum(p.shape[1] for p in parts[::tok_count])
    return pl.pallas_call(
        functools.partial(finish_kernel, tok_count),
        in_specs=[pl.BlockSpec(memory_space=pltpu.SMEM)] * 3
        + [pl.BlockSpec(memory_space=pltpu.VMEM)] * len(parts),
        out_specs=pl.BlockSpec(memory_space=pltpu.VMEM),
        out_shape=jax.ShapeDtypeStruct((slots, share, rank), jnp.float32),
        compiler_params=pltpu.CompilerParams(vmem_limit_bytes=6 * MIB),
        name="finish",
    )(tok, doc_lengths, doc_owner, *parts)


def shards(acts, grads, proj_in, proj_out, doc_lengths, doc_owner):
    rank = proj_in.shape[1]
    tok_count = lax.axis_size("tok")
    feat_count = lax.axis_size("feat")
    chips = feat_count // 2
    feat = lax.axis_index("feat")
    chip = feat // 2
    core = (feat % 2).reshape(1)
    tok = lax.axis_index("tok").reshape(1)
    share = rank // feat_count
    rows = acts.shape[0]
    acts, grads, proj_in, proj_out = (
        pltpu.with_memory_space_constraint(v, pltpu.HBM) for v in (acts, grads, proj_in, proj_out)
    )

    def swap(value):
        return lax.ppermute(value, "feat", partner_pairs(feat_count))

    near, *far = project_grads(grads, proj_out, chip.reshape(1), chips)
    arrived = []
    for step in range(1, chips):
        arrived.append(lax.ppermute(far[step - 1], "feat", chip_shift(feat_count, step)))
    halves = project_acts(acts, proj_in, core, near)

    lows = []
    for chunk in range(CHUNKS):
        mine, theirs = halves[2 * chunk : 2 * chunk + 2]
        other = swap(theirs)
        full_in, sent = vmem_call(
            pair_sum_kernel,
            (),
            (mine, other),
            [pltpu.VMEM(mine.shape, jnp.float32), pltpu.VMEM(mine.shape, jnp.bfloat16)],
        )
        for step in range(1, chips):
            other = lax.ppermute(sent, "feat", chip_shift(feat_count, step))
            full_in = full_in + other.astype(jnp.float32)
        lows.append(full_in.astype(jnp.bfloat16))

    mine, theirs = vmem_call(
        chip_sum_kernel, (core,), (near, *arrived), [pltpu.VMEM((rows, share), jnp.float32)] * 2
    )
    other = swap(theirs)
    spread_low = spread(mine, other, core, tok, doc_lengths, doc_owner, tok_count)
    parts = []
    for low_in in lows:
        other = swap(low_in)
        kept, *sends = outer_products(spread_low, low_in, other, tok_count)
        parts.append(kept)
        for step in range(1, tok_count):
            parts.append(lax.ppermute(sends[step - 1], "tok", exchange(tok_count, step)))
    return finish(parts, tok, doc_lengths, doc_owner, tok_count, share)


def solution(mesh):
    in_specs = (
        P(("grp", "tok"), "feat"),
        P(("grp", "tok"), "feat"),
        P("feat", None),
        P("feat", None),
        P("grp"),
        P("grp"),
    )
    out_specs = P(("grp", "tok"), "feat", None)

    return jax.shard_map(shards, mesh=mesh, in_specs=in_specs, out_specs=out_specs, check_vma=False)
```

```python
import functools

import jax
import jax.numpy as jnp
from jax import lax
from jax.experimental import pallas as pl
from jax.experimental.pallas import tpu as pltpu
from jax.sharding import PartitionSpec as P


CHUNKS = 2
TILE = 512
AHEAD = 8
MIB = 1 << 20


def partner_pairs(size):
    return [(i, i ^ 1) for i in range(size)]


def chip_shift(size, step):
    chips = size // 2
    return [(i, ((i // 2 + step) % chips) * 2 + i % 2) for i in range(size)]


def exchange(size, step):
    if size & (size - 1) == 0:
        return [(i, i ^ step) for i in range(size)]
    return [(i, (i + step) % size) for i in range(size)]


def receiver(size, me, step):
    return me ^ step if size & (size - 1) == 0 else (me + step) % size


def depth_tile(depth, most):
    tile = most // 128 * 128
    while depth % tile:
        tile -= 128
    return tile


def stream(far, near, far_w, near_w, sems):
    depth = near_w.shape[0]
    tile = depth_tile(depth, TILE)
    count = depth // tile

    def lines(t):
        return pl.ds(t * tile, tile)

    def copies(t):
        return (
            pltpu.make_async_copy(far_w.at[lines(t), :], near_w.at[lines(t), :], sems.at[0, t]),
            pltpu.make_async_copy(far.at[:, lines(t)], near.at[:, lines(t)], sems.at[1, t]),
        )

    def start(t):
        for copy in copies(t):
            copy.start()

    for t in range(min(AHEAD, count)):
        start(t)
    for t in range(count):
        for copy in copies(t):
            copy.wait()
        if t + AHEAD < count:
            start(t + AHEAD)
        yield lines(t), t == 0, t + 1 == count


def grads_kernel(chips, chip_ref, a_hbm, w_hbm, near_ref, *refs):
    far_refs, (a_ref, w_ref, total, sems) = refs[:-4], refs[-4:]
    for lines, begins, _ in stream(a_hbm, a_ref, w_hbm, w_ref, sems):
        product = jnp.dot(a_ref[:, lines], w_ref[lines, :], preferred_element_type=jnp.float32)
        if begins:
            total[...] = product
        else:
            total[...] += product
    width = near_ref.shape[1]
    for chip in range(chips):

        @pl.when(chip_ref[0] == chip)
        def _():
            near_ref[...] = total[:, pl.ds(chip * width, width)]
            for step, ref in enumerate(far_refs):
                place = (chip + step + 1) % chips * width
                ref[...] = total[:, pl.ds(place, width)].astype(ref.dtype)


def acts_kernel(core_ref, a_hbm, w_hbm, after_ref, *refs):
    halves, (a_ref, w_ref, total, sems) = refs[:-4], refs[-4:]
    half, width = halves[0].shape
    for lines, begins, ends in stream(a_hbm, a_ref, w_hbm, w_ref, sems):
        if not ends:
            product = jnp.dot(a_ref[:, lines], w_ref[lines, :], preferred_element_type=jnp.float32)
            if begins:
                total[...] = product
            else:
                total[...] += product
            continue
        for side in range(2):
            place = core_ref[0] if side == 0 else 1 - core_ref[0]
            rows = pl.ds(pl.multiple_of(place * half, half), half)
            result = jnp.dot(a_ref[rows, lines], w_ref[lines, :], preferred_element_type=jnp.float32)
            if not begins:
                result = total[rows, :] + result
            for chunk in range(len(halves) // 2):
                halves[2 * chunk + side][...] = result[:, chunk * width : (chunk + 1) * width]


def product_call(kernel, scalar, a, w, after, out):
    rows, depth = a.shape
    rank = w.shape[1]
    return pl.pallas_call(
        kernel,
        in_specs=[pl.BlockSpec(memory_space=pltpu.SMEM)]
        + [pl.BlockSpec(memory_space=pltpu.HBM)] * 2
        + [pl.BlockSpec(memory_space=pl.ANY)] * len(after),
        out_specs=[pl.BlockSpec(memory_space=pltpu.VMEM)] * len(out),
        out_shape=out,
        scratch_shapes=[
            pltpu.VMEM((rows, depth), a.dtype),
            pltpu.VMEM((depth, rank), w.dtype),
            pltpu.VMEM((rows, rank), jnp.float32),
            pltpu.SemaphoreType.DMA((2, depth // depth_tile(depth, TILE))),
        ],
        compiler_params=pltpu.CompilerParams(
            vmem_limit_bytes=2 * depth * (rows + rank) + 4 * rows * rank + 3 * MIB
        ),
        cost_estimate=pl.CostEstimate(
            flops=2 * rows * depth * rank,
            bytes_accessed=2 * (rows + rank) * depth,
            transcendentals=0,
        ),
    )(scalar, a, w, *after)


def project_grads(grads, proj_out, chip, chips):
    rows, rank = grads.shape[0], proj_out.shape[1]
    width = rank // chips
    out = [pltpu.VMEM((rows, width), jnp.float32)]
    out += [pltpu.VMEM((rows, width), jnp.bfloat16)] * (chips - 1)
    return product_call(functools.partial(grads_kernel, chips), chip, grads, proj_out, [], out)


def project_acts(acts, proj_in, core, after):
    rows, rank = acts.shape[0], proj_in.shape[1]
    out = [pltpu.VMEM((rows // 2, rank // CHUNKS), jnp.float32)] * (2 * CHUNKS)
    return product_call(acts_kernel, core, acts, proj_in, [after], out)


def vmem_call(kernel, scalars, arrays, out, limit=6, flops=10**5):
    arrays = [pltpu.with_memory_space_constraint(v, pltpu.VMEM) for v in arrays]
    return pl.pallas_call(
        kernel,
        in_specs=[pl.BlockSpec(memory_space=pltpu.SMEM)] * len(scalars)
        + [pl.BlockSpec(memory_space=pltpu.VMEM)] * len(arrays),
        out_specs=[pl.BlockSpec(memory_space=pltpu.VMEM)] * len(out),
        out_shape=out,
        compiler_params=pltpu.CompilerParams(vmem_limit_bytes=limit * MIB),
        cost_estimate=pl.CostEstimate(flops=flops, bytes_accessed=0, transcendentals=0),
    )(*scalars, *arrays)


def chip_sum_kernel(core_ref, near_ref, *refs):
    far_refs, (mine_ref, theirs_ref) = refs[:-2], refs[-2:]
    share = mine_ref.shape[1]
    for which in range(2):

        @pl.when(core_ref[0] == which)
        def _():
            for side, out_ref in ((which, mine_ref), (1 - which, theirs_ref)):
                place = pl.ds(side * share, share)
                total = near_ref[:, place]
                for ref in far_refs:
                    total = total + ref[:, place].astype(jnp.float32)
                out_ref[...] = total


def pair_sum_kernel(mine_ref, other_ref, total_ref, sent_ref):
    total = mine_ref[...] + other_ref[...]
    total_ref[...] = total
    sent_ref[...] = total.astype(sent_ref.dtype)


def spread_kernel(
    tok_count, core_ref, tok_ref, lengths_ref, owner_ref, mine_ref, other_ref, out_ref, scale_ref
):
    rows, share = mine_ref.shape
    docs = lengths_ref.shape[0]
    slots = docs // tok_count
    half = rows // 2
    tok, core = tok_ref[0], core_ref[0]
    starts, ends, targets = [], [], []
    seen = jnp.int32(0)
    for d in range(docs):
        starts.append(seen)
        seen = seen + lengths_ref[d]
        ends.append(seen)
        rank = jnp.int32(0)
        for e in range(d):
            rank = rank + (owner_ref[e] == owner_ref[d]).astype(jnp.int32)
        targets.append(owner_ref[d] * slots + rank)
    for slot in range(slots):
        length = jnp.int32(1)
        for d in range(docs):
            length = jnp.where(targets[d] == tok * slots + slot, lengths_ref[d], length)
        length = jnp.full((8, 128), length, jnp.int32).astype(jnp.float32)
        scale_ref[pl.ds(slot * 8, 8), :] = lax.rsqrt(length)
    low = (mine_ref[...] + other_ref[...]).astype(jnp.bfloat16)
    turned = low.astype(jnp.float32).T
    for part in range(2):
        first = (core if part == 0 else 1 - core) * half
        position = tok * rows + first + lax.broadcasted_iota(jnp.int32, (share, half), 1)
        piece = jnp.where(
            core == part, turned[:, :half], turned[:, half:]
        )
        for step in range(tok_count):
            for slot in range(slots):
                want = receiver(tok_count, tok, step) * slots + slot
                begin = end = jnp.int32(0)
                for d in range(docs):
                    hit = targets[d] == want
                    begin = jnp.where(hit, starts[d], begin)
                    end = jnp.where(hit, ends[d], end)
                member = (position >= begin) & (position < end)
                out_ref[pl.ds((step * slots + slot) * share, share), pl.ds(part * half, half)] = (
                    jnp.where(member, piece, 0.0).astype(out_ref.dtype)
                )


def spread(mine, other, core, tok, doc_lengths, doc_owner, tok_count):
    rows, share = mine.shape
    docs = doc_lengths.shape[0]
    return vmem_call(
        functools.partial(spread_kernel, tok_count),
        (core, tok, doc_lengths, doc_owner),
        (mine, other),
        [
            pltpu.VMEM((docs * share, rows), jnp.bfloat16),
            pltpu.VMEM((docs // tok_count * 8, 128), jnp.float32),
        ],
        limit=8,
    )


def product_kernel(w_ref, own_ref, other_ref, kept_ref, *sent_refs):
    half = own_ref.shape[0]
    size = kept_ref.shape[0]
    product = jnp.dot(w_ref[:, :half], own_ref[...], preferred_element_type=jnp.float32)
    product += jnp.dot(w_ref[:, half:], other_ref[...], preferred_element_type=jnp.float32)
    kept_ref[...] = product[:size]
    for i, ref in enumerate(sent_refs):
        ref[...] = product[(i + 1) * size : (i + 2) * size].astype(ref.dtype)


def outer_products(spread_low, own, other, tok_count):
    size = spread_low.shape[0] // tok_count
    width = own.shape[1]
    return pl.pallas_call(
        product_kernel,
        in_specs=[pl.BlockSpec(memory_space=pltpu.VMEM)] * 3,
        out_specs=[pl.BlockSpec(memory_space=pltpu.VMEM)] * tok_count,
        out_shape=[pltpu.VMEM((size, width), jnp.float32)]
        + [pltpu.VMEM((size, width), jnp.bfloat16)] * (tok_count - 1),
        compiler_params=pltpu.CompilerParams(vmem_limit_bytes=6 * MIB),
        cost_estimate=pl.CostEstimate(
            flops=2 * spread_low.shape[0] * spread_low.shape[1] * width,
            bytes_accessed=0,
            transcendentals=0,
        ),
        name="outer_products",
    )(spread_low, own, other)


def finish_kernel(tok_count, scale_ref, *refs):
    total_refs, out_ref = refs[:-1], refs[-1]
    slots, share, _ = out_ref.shape
    for slot in range(slots):
        scale = jnp.broadcast_to(scale_ref[pl.ds(slot * 8, 1), :], (share, 128))
        lines = pl.ds(slot * share, share)
        place = 0
        for chunk in range(CHUNKS):
            parts = total_refs[chunk * tok_count : (chunk + 1) * tok_count]
            for begin in range(0, parts[0].shape[1], 128):
                columns = pl.ds(begin, 128)
                total = parts[0][lines, columns]
                for part in parts[1:]:
                    total = total + part[lines, columns].astype(jnp.float32)
                out_ref[slot, :, pl.ds(place, 128)] = total * scale
                place += 128


def finish(parts, scale, tok_count, slots, share):
    rank = sum(p.shape[1] for p in parts[::tok_count])
    out = [jax.ShapeDtypeStruct((slots, share, rank), jnp.float32)]
    (result,) = vmem_call(functools.partial(finish_kernel, tok_count), (), (scale, *parts), out)
    return result


def shards(acts, grads, proj_in, proj_out, doc_lengths, doc_owner):
    rank = proj_in.shape[1]
    tok_count = lax.axis_size("tok")
    feat_count = lax.axis_size("feat")
    chips = feat_count // 2
    feat = lax.axis_index("feat")
    chip = feat // 2
    core = (feat % 2).reshape(1)
    tok = lax.axis_index("tok").reshape(1)
    share = rank // feat_count
    rows = acts.shape[0]
    acts, grads, proj_in, proj_out = (
        pltpu.with_memory_space_constraint(v, pltpu.HBM) for v in (acts, grads, proj_in, proj_out)
    )

    def swap(value):
        return lax.ppermute(value, "feat", partner_pairs(feat_count))

    near, *far = project_grads(grads, proj_out, chip.reshape(1), chips)
    arrived = []
    for step in range(1, chips):
        arrived.append(lax.ppermute(far[step - 1], "feat", chip_shift(feat_count, step)))
    halves = project_acts(acts, proj_in, core, near)

    lows = []
    for chunk in range(CHUNKS):
        mine, theirs = halves[2 * chunk : 2 * chunk + 2]
        other = swap(theirs)
        full_in, sent = vmem_call(
            pair_sum_kernel,
            (),
            (mine, other),
            [pltpu.VMEM(mine.shape, jnp.float32), pltpu.VMEM(mine.shape, jnp.bfloat16)],
        )
        for step in range(1, chips):
            other = lax.ppermute(sent, "feat", chip_shift(feat_count, step))
            full_in = full_in + other.astype(jnp.float32)
        lows.append(full_in.astype(jnp.bfloat16))

    mine, theirs = vmem_call(
        chip_sum_kernel, (core,), (near, *arrived), [pltpu.VMEM((rows, share), jnp.float32)] * 2
    )
    other = swap(theirs)
    spread_low, scale = spread(mine, other, core, tok, doc_lengths, doc_owner, tok_count)
    parts = []
    for low_in in lows:
        other = swap(low_in)
        kept, *sends = outer_products(spread_low, low_in, other, tok_count)
        parts.append(kept)
        for step in range(1, tok_count):
            parts.append(lax.ppermute(sends[step - 1], "tok", exchange(tok_count, step)))
    return finish(parts, scale, tok_count, doc_lengths.shape[0] // tok_count, share)


def solution(mesh):
    in_specs = (
        P(("grp", "tok"), "feat"),
        P(("grp", "tok"), "feat"),
        P("feat", None),
        P("feat", None),
        P("grp"),
        P("grp"),
    )
    out_specs = P(("grp", "tok"), "feat", None)

    return jax.shard_map(shards, mesh=mesh, in_specs=in_specs, out_specs=out_specs, check_vma=False)
```

```python
import functools

import jax
import jax.numpy as jnp
from jax import lax
from jax.experimental import pallas as pl
from jax.experimental.pallas import tpu as pltpu
from jax.sharding import PartitionSpec as P


CHUNKS = 2
TILE = 512
NEAR_TILE = 1024
NEAR_AHEAD = 4
AHEAD = 8
MIB = 1 << 20


def partner_pairs(size):
    return [(i, i ^ 1) for i in range(size)]


def chip_shift(size, step):
    chips = size // 2
    return [(i, ((i // 2 + step) % chips) * 2 + i % 2) for i in range(size)]


def exchange(size, step):
    if size & (size - 1) == 0:
        return [(i, i ^ step) for i in range(size)]
    return [(i, (i + step) % size) for i in range(size)]


def receiver(size, me, step):
    return me ^ step if size & (size - 1) == 0 else (me + step) % size


def depth_tile(depth, most):
    tile = most // 128 * 128
    while depth % tile:
        tile -= 128
    return tile


def tiles(depth, most):
    tile = depth_tile(depth, most)
    lengths = [tile] * (depth // tile)
    if tile % 512 == 0 and tile > 512:
        lengths[:1] = [tile // 4, tile // 4, tile // 2]
    return [(sum(lengths[:t]), length) for t, length in enumerate(lengths)]


def stream(far, near, far_w, near_w, sems, most, ahead):
    lines = [pl.ds(begin, length) for begin, length in tiles(near_w.shape[0], most)]

    def copies(t):
        pair = [pltpu.make_async_copy(far.at[:, lines[t]], near.at[:, lines[t]], sems.at[1, t])]
        if far_w is not None:
            pair.append(
                pltpu.make_async_copy(far_w.at[lines[t], :], near_w.at[lines[t], :], sems.at[0, t])
            )
        return pair

    def start(t):
        for copy in copies(t):
            copy.start()

    for t in range(min(ahead, len(lines))):
        start(t)
    for t in range(len(lines)):
        for copy in copies(t):
            copy.wait()
        if t + ahead < len(lines):
            start(t + ahead)
        yield lines[t], t == 0, t + 1 == len(lines)


def grads_kernel(chips, a_hbm, w_hbm, near_ref, *refs):
    far_refs, (a_ref, w_ref, total, sems) = refs[:-4], refs[-4:]
    for lines, begins, _ in stream(a_hbm, a_ref, w_hbm, w_ref, sems, TILE, AHEAD):
        product = jnp.dot(a_ref[:, lines], w_ref[lines, :], preferred_element_type=jnp.float32)
        if begins:
            total[...] = product
        else:
            total[...] += product
    width = near_ref.shape[1]
    for chip in range(chips):

        @pl.when(lax.axis_index("feat") // 2 == chip)
        def _():
            near_ref[...] = total[:, pl.ds(chip * width, width)]
            for step, ref in enumerate(far_refs):
                place = (chip + step + 1) % chips * width
                ref[...] = total[:, pl.ds(place, width)].astype(ref.dtype)


def acts_kernel(a_hbm, w_ref, after_ref, *refs):
    core = lax.rem(lax.axis_index("feat"), 2)
    halves, (a_ref, _, total, sems) = refs[:-4], refs[-4:]
    half, width = halves[0].shape
    for lines, begins, ends in stream(a_hbm, a_ref, None, w_ref, sems, NEAR_TILE, NEAR_AHEAD):
        if not ends:
            product = jnp.dot(a_ref[:, lines], w_ref[lines, :], preferred_element_type=jnp.float32)
            if begins:
                total[...] = product
            else:
                total[...] += product
            continue
        for chunk in range(len(halves) // 2):
            columns = pl.ds(chunk * width, width)
            for side in range(2):
                place = core if side == 0 else 1 - core
                rows = pl.ds(pl.multiple_of(place * half, half), half)
                result = jnp.dot(
                    a_ref[rows, lines], w_ref[lines, columns], preferred_element_type=jnp.float32
                )
                if not begins:
                    result = total[rows, columns] + result
                halves[2 * chunk + side][...] = result


def product_call(kernel, a, w, after, out):
    rows, depth = a.shape
    rank = w.shape[1]
    return pl.pallas_call(
        kernel,
        in_specs=[pl.BlockSpec(memory_space=pltpu.HBM)]
        + [pl.BlockSpec(memory_space=pltpu.VMEM if after else pltpu.HBM)]
        + [pl.BlockSpec(memory_space=pl.ANY)] * len(after),
        out_specs=[pl.BlockSpec(memory_space=pltpu.VMEM)] * len(out),
        out_shape=out,
        scratch_shapes=[
            pltpu.VMEM((rows, depth), a.dtype),
            pltpu.VMEM((8, rank) if after else (depth, rank), w.dtype),
            pltpu.VMEM((rows, rank), jnp.float32),
            pltpu.SemaphoreType.DMA((2, len(tiles(depth, NEAR_TILE if after else TILE)))),
        ],
        compiler_params=pltpu.CompilerParams(
            vmem_limit_bytes=2 * depth * (rows + (0 if after else rank)) + 4 * rows * rank + 3 * MIB
        ),
        cost_estimate=pl.CostEstimate(
            flops=2 * rows * depth * rank * (1 if after else 10),
            bytes_accessed=0,
            transcendentals=0,
        ),
    )(a, w, *after)


def project_grads(grads, proj_out, chips):
    rows, rank = grads.shape[0], proj_out.shape[1]
    width = rank // chips
    out = [pltpu.VMEM((rows, width), jnp.float32)]
    out += [pltpu.VMEM((rows, width), jnp.bfloat16)] * (chips - 1)
    return product_call(functools.partial(grads_kernel, chips), grads, proj_out, [], out)


def project_acts(acts, proj_in, after):
    rows, rank = acts.shape[0], proj_in.shape[1]
    out = [pltpu.VMEM((rows // 2, rank // CHUNKS), jnp.float32)] * (2 * CHUNKS)
    return product_call(acts_kernel, acts, proj_in, [after], out)


def vmem_call(kernel, scalars, arrays, out, limit=6, flops=10**5):
    arrays = [pltpu.with_memory_space_constraint(v, pltpu.VMEM) for v in arrays]
    return pl.pallas_call(
        kernel,
        in_specs=[pl.BlockSpec(memory_space=pltpu.SMEM)] * len(scalars)
        + [pl.BlockSpec(memory_space=pltpu.VMEM)] * len(arrays),
        out_specs=[pl.BlockSpec(memory_space=pltpu.VMEM)] * len(out),
        out_shape=out,
        compiler_params=pltpu.CompilerParams(vmem_limit_bytes=limit * MIB),
        cost_estimate=pl.CostEstimate(flops=flops, bytes_accessed=0, transcendentals=0),
    )(*scalars, *arrays)


def chip_sum_kernel(near_ref, *refs):
    far_refs, (mine_ref, theirs_ref) = refs[:-2], refs[-2:]
    share = mine_ref.shape[1]
    for which in range(2):

        @pl.when(lax.rem(lax.axis_index("feat"), 2) == which)
        def _():
            for side, out_ref in ((which, mine_ref), (1 - which, theirs_ref)):
                place = pl.ds(side * share, share)
                total = near_ref[:, place]
                for ref in far_refs:
                    total = total + ref[:, place].astype(jnp.float32)
                out_ref[...] = total


def pair_sum_kernel(mine_ref, other_ref, total_ref, sent_ref):
    total = mine_ref[...] + other_ref[...]
    total_ref[...] = total
    sent_ref[...] = total.astype(sent_ref.dtype)


def spread_kernel(
    tok_count, lengths_ref, owner_ref, mine_ref, other_ref, out_ref, scale_ref
):
    rows, share = mine_ref.shape
    docs = lengths_ref.shape[0]
    slots = docs // tok_count
    half = rows // 2
    tok, core = lax.axis_index("tok"), lax.rem(lax.axis_index("feat"), 2)
    starts, ends, targets = [], [], []
    seen = jnp.int32(0)
    for d in range(docs):
        starts.append(seen)
        seen = seen + lengths_ref[d]
        ends.append(seen)
        rank = jnp.int32(0)
        for e in range(d):
            rank = rank + (owner_ref[e] == owner_ref[d]).astype(jnp.int32)
        targets.append(owner_ref[d] * slots + rank)
    for slot in range(slots):
        length = jnp.int32(1)
        for d in range(docs):
            length = jnp.where(targets[d] == tok * slots + slot, lengths_ref[d], length)
        length = jnp.full((8, 128), length, jnp.int32).astype(jnp.float32)
        scale_ref[pl.ds(slot * 8, 8), :] = lax.rsqrt(length)
    low = (mine_ref[...] + other_ref[...]).astype(jnp.bfloat16)
    turned = low.astype(jnp.float32).T
    for part in range(2):
        first = (core if part == 0 else 1 - core) * half
        position = tok * rows + first + lax.broadcasted_iota(jnp.int32, (share, half), 1)
        piece = jnp.where(
            core == part, turned[:, :half], turned[:, half:]
        )
        for step in range(tok_count):
            for slot in range(slots):
                want = receiver(tok_count, tok, step) * slots + slot
                begin = end = jnp.int32(0)
                for d in range(docs):
                    hit = targets[d] == want
                    begin = jnp.where(hit, starts[d], begin)
                    end = jnp.where(hit, ends[d], end)
                member = (position >= begin) & (position < end)
                out_ref[pl.ds((step * slots + slot) * share, share), pl.ds(part * half, half)] = (
                    jnp.where(member, piece, 0.0).astype(out_ref.dtype)
                )


def spread(mine, other, doc_lengths, doc_owner, tok_count):
    rows, share = mine.shape
    docs = doc_lengths.shape[0]
    return vmem_call(
        functools.partial(spread_kernel, tok_count),
        (doc_lengths, doc_owner),
        (mine, other),
        [
            pltpu.VMEM((docs * share, rows), jnp.bfloat16),
            pltpu.VMEM((docs // tok_count * 8, 128), jnp.float32),
        ],
        limit=8,
    )


def product_kernel(w_ref, own_ref, other_ref, kept_ref, *sent_refs):
    half = own_ref.shape[0]
    size = kept_ref.shape[0]
    product = jnp.dot(w_ref[:, :half], own_ref[...], preferred_element_type=jnp.float32)
    product += jnp.dot(w_ref[:, half:], other_ref[...], preferred_element_type=jnp.float32)
    kept_ref[...] = product[:size]
    for i, ref in enumerate(sent_refs):
        ref[...] = product[(i + 1) * size : (i + 2) * size].astype(ref.dtype)


def outer_products(spread_low, own, other, tok_count):
    size = spread_low.shape[0] // tok_count
    width = own.shape[1]
    return pl.pallas_call(
        product_kernel,
        in_specs=[pl.BlockSpec(memory_space=pltpu.VMEM)] * 3,
        out_specs=[pl.BlockSpec(memory_space=pltpu.VMEM)] * tok_count,
        out_shape=[pltpu.VMEM((size, width), jnp.float32)]
        + [pltpu.VMEM((size, width), jnp.bfloat16)] * (tok_count - 1),
        compiler_params=pltpu.CompilerParams(vmem_limit_bytes=6 * MIB),
        cost_estimate=pl.CostEstimate(
            flops=2 * spread_low.shape[0] * spread_low.shape[1] * width,
            bytes_accessed=0,
            transcendentals=0,
        ),
        name="outer_products",
    )(spread_low, own, other)


def finish_kernel(tok_count, scale_ref, *refs):
    total_refs, out_ref = refs[:-1], refs[-1]
    slots, share, _ = out_ref.shape
    for slot in range(slots):
        scale = jnp.broadcast_to(scale_ref[pl.ds(slot * 8, 1), :], (share, 128))
        lines = pl.ds(slot * share, share)
        place = 0
        for chunk in range(CHUNKS):
            parts = total_refs[chunk * tok_count : (chunk + 1) * tok_count]
            for begin in range(0, parts[0].shape[1], 128):
                columns = pl.ds(begin, 128)
                total = parts[0][lines, columns]
                for part in parts[1:]:
                    total = total + part[lines, columns].astype(jnp.float32)
                out_ref[slot, :, pl.ds(place, 128)] = total * scale
                place += 128


def finish(parts, scale, tok_count, slots, share):
    rank = sum(p.shape[1] for p in parts[::tok_count])
    out = [jax.ShapeDtypeStruct((slots, share, rank), jnp.float32)]
    (result,) = vmem_call(functools.partial(finish_kernel, tok_count), (), (scale, *parts), out)
    return result


def shards(acts, grads, proj_in, proj_out, doc_lengths, doc_owner):
    rank = proj_in.shape[1]
    tok_count = lax.axis_size("tok")
    feat_count = lax.axis_size("feat")
    chips = feat_count // 2
    share = rank // feat_count
    rows = acts.shape[0]
    acts, grads, proj_out = (
        pltpu.with_memory_space_constraint(v, pltpu.HBM) for v in (acts, grads, proj_out)
    )

    def swap(value):
        return lax.ppermute(value, "feat", partner_pairs(feat_count))

    near, *far = project_grads(grads, proj_out, chips)
    arrived = []
    for step in range(1, chips):
        arrived.append(lax.ppermute(far[step - 1], "feat", chip_shift(feat_count, step)))
    halves = project_acts(acts, proj_in, near)

    lows = []
    for chunk in range(CHUNKS):
        mine, theirs = halves[2 * chunk : 2 * chunk + 2]
        other = swap(theirs)
        full_in, sent = vmem_call(
            pair_sum_kernel,
            (),
            (mine, other),
            [pltpu.VMEM(mine.shape, jnp.float32), pltpu.VMEM(mine.shape, jnp.bfloat16)],
        )
        for step in range(1, chips):
            other = lax.ppermute(sent, "feat", chip_shift(feat_count, step))
            full_in = full_in + other.astype(jnp.float32)
        lows.append(full_in.astype(jnp.bfloat16))

    mine, theirs = vmem_call(
        chip_sum_kernel, (), (near, *arrived), [pltpu.VMEM((rows, share), jnp.float32)] * 2
    )
    other = swap(theirs)
    spread_low, scale = spread(mine, other, doc_lengths, doc_owner, tok_count)
    parts = []
    for low_in in lows:
        other = swap(low_in)
        kept, *sends = outer_products(spread_low, low_in, other, tok_count)
        parts.append(kept)
        for step in range(1, tok_count):
            parts.append(lax.ppermute(sends[step - 1], "tok", exchange(tok_count, step)))
    return finish(parts, scale, tok_count, doc_lengths.shape[0] // tok_count, share)


def solution(mesh):
    in_specs = (
        P(("grp", "tok"), "feat"),
        P(("grp", "tok"), "feat"),
        P("feat", None),
        P("feat", None),
        P("grp"),
        P("grp"),
    )
    out_specs = P(("grp", "tok"), "feat", None)

    return jax.shard_map(shards, mesh=mesh, in_specs=in_specs, out_specs=out_specs, check_vma=False)
```
